32 devices in a mesh: tok: 8 (over z, y), voc: 4 (over x, core).
Axes of the slice: x: 2, y: 2, z: 4, core: 2. Of those that a mesh axis runs over, the one named last changes fastest.
Arguments:
- hidden: bfloat16 [1024, 3584], P('tok', 'voc'), may hold values from -36 to 36
- weight: bfloat16 [3584, 256000], P(None, ('voc', 'tok')), may hold values from -1 to 1
- targets: int32 [1024], replicated, may hold values from 0 to 255999
- slot: int32 [8], replicated, may hold values from 0 to 7, each once
- prompt_len: int32 [8], replicated, may hold values from 1 to 64
- ref_means: float32 [8], replicated, may hold values from -17 to -13
Outputs:
- token_logprobs: float32 [1024], P('tok')
- margins: float32 [4], replicated
- loss: float32 [], replicated
The draws below stay inside these ranges and needn't reach their ends.
All inputs are finite; a program needn't handle non-finite values.
Results may differ from the reference program's by a relative error of at most 0.0003.
Values may be sent and summed in bfloat16 or wider, within the bound.
A program may use at most 192 MiB of HBM per device.

```python
import math
import jax
import jax.numpy as jnp
import numpy as np
from jax import lax

D = 3584
V = 256000
SEQLEN = 128
TOKENS = 1024
SEQS = 8


def weight_block(key, blk_id):
    weight_key = jax.random.fold_in(key, 11)
    return jnp.clip(jax.random.normal(jax.random.fold_in(weight_key, blk_id), (D, 128), jnp.float32), -5.0, 5.0)


def draw_weight(key, part):
    blocks = jax.vmap(lambda blk_id: weight_block(key, blk_id))(jnp.arange(V // 128, dtype=jnp.int32))
    whole = jnp.transpose(blocks, (1, 0, 2)).reshape(D, V)
    whole = jnp.clip(whole / math.sqrt(D), -1.0, 1.0)
    return whole.astype(jnp.bfloat16)


def draw_hidden(key, part):
    base = jnp.clip(jax.random.normal(jax.random.fold_in(key, 21), (TOKENS, D), jnp.float32), -5.0, 5.0)
    values = 3.0 * base
    return values.astype(jnp.bfloat16)


def place_ends(result, own_key, least, top_value):
    shape = result.shape
    index_at = [jax.random.randint(jax.random.fold_in(own_key, axis), (), 0, shape[axis]) for axis in range(len(shape))]
    result = result.at[tuple(index_at)].set(least)
    longest = shape.index(max(shape))
    index_at[longest] = (index_at[longest] + 1) % shape[longest]
    return result.at[tuple(index_at)].set(top_value)


def skewed_wide(rng, dims, number_of, skew):
    weights = [min(1 << octave, number_of + 1 - (1 << octave)) * (1 << 20) // math.isqrt((1 << octave) ** skew) + 1 for octave in range((number_of + 1).bit_length()) if 1 << octave <= number_of]
    deviation = 1 + sum(weights) // (1 << 30)
    grid = np.cumsum(np.array([max(1, weight // deviation) for weight in weights]))
    lot = jax.random.randint(jax.random.fold_in(rng, 1), dims, 0, int(grid[len(weights) - 1]))
    start = jnp.left_shift(1, jnp.searchsorted(jnp.asarray(grid, jnp.int32), lot, side="right").astype(jnp.int32))
    rank = start - 1 + jax.random.randint(jax.random.fold_in(rng, 4), dims, 0, 1 << 30) % jnp.minimum(start, number_of + 1 - start)
    return jax.random.permutation(jax.random.fold_in(rng, 2), number_of)[rank].astype(jnp.int32)


def setup_inputs(seed: int = 0) -> dict:
    key_list = jax.random.split(jax.random.key(seed), 7)
    return {
        "hidden": draw_hidden(jax.random.fold_in(key_list[6], 71), 0),
        "weight": draw_weight(jax.random.fold_in(key_list[6], 71), 0),
        "targets": place_ends(skewed_wide(key_list[2], (TOKENS,), V, 2), jax.random.fold_in(key_list[2], 3), 0, V - 1).astype(jnp.int32),
        "slot": jax.random.permutation(key_list[3], SEQS).astype(jnp.int32),
        "prompt_len": place_ends(jax.random.randint(key_list[4], (SEQS,), 1, SEQLEN // 2 + 1), jax.random.fold_in(key_list[4], 1), 1, (SEQLEN // 2 + 1) - 1).astype(jnp.int32),
        "ref_means": jnp.clip(jax.random.uniform(key_list[5], (SEQS,), jnp.float32, -17.0, -13.0), -17.0, -13.0),
    }


beta_scale = 2.0


def finish(token_lp, slot, prompt_len, ref_means):
    seq_count = slot.shape[0]
    per_seq = token_lp.reshape(seq_count, -1)
    seq_width = per_seq.shape[1]
    position = jnp.arange(seq_width, dtype=jnp.int32)[None, :]
    in_reply = position >= prompt_len[:, None]
    reply_len = (seq_width - prompt_len).astype(jnp.float32)
    seq_means = jnp.sum(jnp.where(in_reply, per_seq, jnp.float32(0.0)), axis=1) / reply_len
    advantage = seq_means - ref_means
    polarity = jnp.where(slot % 2 == 0, jnp.float32(1.0), jnp.float32(-1.0))
    n_pairs = seq_count // 2
    onehot = (slot[:, None] // 2) == jnp.arange(n_pairs, dtype=jnp.int32)[None, :]
    signed = (polarity * advantage)[:, None]
    margins = beta_scale * jnp.sum(jnp.where(onehot, signed, jnp.float32(0.0)), axis=0)
    pair_loss = jnp.mean(jax.nn.softplus(-margins))
    return margins, pair_loss


def reference(hidden, weight, targets, slot, prompt_len, ref_means):
    blocks = hidden.reshape(TOKENS // SEQLEN, SEQLEN, D)
    target_blocks = targets.reshape(TOKENS // SEQLEN, SEQLEN)

    def one_block(operands):
        rows_h, rows_t = operands
        logits = jnp.dot(rows_h, weight, preferred_element_type=jnp.float32)
        row_max = jnp.max(logits, axis=1)
        row_sum = jnp.sum(jnp.exp(logits - row_max[:, None]), axis=1)
        picked = jnp.take_along_axis(logits, rows_t[:, None].astype(jnp.int32), axis=1)[:, 0]
        return picked - (row_max + jnp.log(row_sum))

    token_lp = lax.map(one_block, (blocks, target_blocks)).reshape(TOKENS)
    margins, pair_loss = finish(token_lp, slot, prompt_len, ref_means)
    return token_lp, margins, pair_loss
```

```python
import functools

import jax
import jax.numpy as jnp
from jax import lax
from jax.experimental import pallas as pl
from jax.experimental.pallas import tpu as pltpu
from jax.sharding import PartitionSpec as P

beta_scale = 2.0
LOW = -1e30
LANES = 128
SUBS = 8
TILE = 512
CHUNK = 64
NT = (((1,), (1,)), ((), ()))


def stats_pass(x_ref, tgt_ref, m_ref, s_ref, t_ref, base, cols):
    lane = lax.broadcasted_iota(jnp.int32, (CHUNK, LANES), 1)
    for r in range(0, x_ref.shape[0], CHUNK):
        rows = pl.ds(r, CHUNK)
        wanted = tgt_ref[rows, :] - base
        xs = []
        for k in range(TILE // LANES):
            x = x_ref[rows, k * LANES : (k + 1) * LANES]
            xs.append(jnp.where(lane < cols - base - k * LANES, x, LOW))
        m_old = m_ref[rows, :]
        m_new = functools.reduce(jnp.maximum, xs, m_old)
        s = s_ref[rows, :] * jnp.exp(m_old - m_new)
        t = t_ref[rows, :]
        for k, x in enumerate(xs):
            s = s + jnp.exp(x - m_new)
            t = t + jnp.where(wanted == lane + k * LANES, x, 0.0)
        m_ref[rows, :] = m_new
        s_ref[rows, :] = s
        t_ref[rows, :] = t


def logits_kernel(cols, h_ref, w_ref, tgt_ref, out_ref, a_ref, b_ref, m_ref, s_ref, t_ref):
    step = pl.program_id(0)

    @pl.when(step == 0)
    def _():
        b_ref[...] = jnp.full_like(b_ref, LOW)
        m_ref[...] = jnp.full_like(m_ref, LOW)
        s_ref[...] = jnp.zeros_like(s_ref)
        t_ref[...] = jnp.zeros_like(t_ref)

    base = step * (2 * TILE)
    fold = functools.partial(stats_pass, tgt_ref=tgt_ref, m_ref=m_ref, s_ref=s_ref, t_ref=t_ref, cols=cols)
    a_ref[...] = lax.dot_general(h_ref[...], w_ref[:TILE], NT, preferred_element_type=jnp.float32)
    fold(b_ref, base=base - TILE)
    b_ref[...] = lax.dot_general(h_ref[...], w_ref[TILE:], NT, preferred_element_type=jnp.float32)
    fold(a_ref, base=base)

    @pl.when(step == pl.num_programs(0) - 1)
    def _():
        fold(b_ref, base=base + TILE)
        diagonal = lax.broadcasted_iota(jnp.int32, (LANES, LANES), 0) == lax.broadcasted_iota(jnp.int32, (LANES, LANES), 1)
        for q in range(out_ref.shape[1]):
            rows = pl.ds(q * LANES, LANES)
            m = m_ref[rows, :]
            top = jnp.max(m, axis=1, keepdims=True)
            total = jnp.sum(s_ref[rows, :] * jnp.exp(m - top), axis=1, keepdims=True)
            lse = top + jnp.log(total)
            hit = jnp.sum(t_ref[rows, :], axis=1, keepdims=True)
            out_ref[0, pl.ds(q, 1), :] = jnp.sum(jnp.where(diagonal, lse, 0.0), axis=0, keepdims=True)
            out_ref[1, pl.ds(q, 1), :] = jnp.sum(jnp.where(diagonal, hit, 0.0), axis=0, keepdims=True)


def local_stats(full, weight, wanted):
    rows, depth = full.shape
    cols = weight.shape[0]
    steps = pl.cdiv(cols, 2 * TILE)
    whole = lambda i: (0, 0)
    return pl.pallas_call(
        functools.partial(logits_kernel, cols),
        grid=(steps,),
        out_shape=jax.ShapeDtypeStruct((2, rows // LANES, LANES), jnp.float32),
        in_specs=[
            pl.BlockSpec((rows, depth), whole),
            pl.BlockSpec((2 * TILE, depth), lambda i: (i, 0)),
            pl.BlockSpec((rows, LANES), whole),
        ],
        out_specs=pl.BlockSpec((2, rows // LANES, LANES), lambda i: (0, 0, 0)),
        scratch_shapes=[pltpu.VMEM((rows, TILE), jnp.float32)] * 2 + [pltpu.VMEM((rows, LANES), jnp.float32)] * 3,
        compiler_params=pltpu.CompilerParams(vmem_limit_bytes=62 * 1024 * 1024, dimension_semantics=("arbitrary",)),
        cost_estimate=pl.CostEstimate(flops=2 * rows * depth * cols, bytes_accessed=2 * depth * (rows + cols), transcendentals=rows * cols),
    )(full, weight, wanted)


def finish_kernel(n_tok, n_dev, stats_ref, slot_ref, prompt_ref, ref_ref, own_ref, margin_ref, loss_ref, got, send_sem, recv_sem):
    me = lax.axis_index("voc") * n_tok + lax.axis_index("tok")

    def peer(k):
        other = lax.rem(me + k, n_dev)
        return {"tok": lax.rem(other, n_tok), "voc": lax.div(other, n_tok)}

    barrier = pltpu.get_barrier_semaphore()

    @pl.loop(1, n_dev)
    def _(k):
        pl.semaphore_signal(barrier, inc=1, device_id=peer(k), device_id_type=pl.DeviceIdType.MESH)

    pl.semaphore_wait(barrier, n_dev - 1)

    def copy(k, source):
        return pltpu.make_async_remote_copy(
            src_ref=stats_ref,
            dst_ref=got.at[source],
            send_sem=send_sem.at[k],
            recv_sem=recv_sem.at[k],
            device_id=peer(k),
            device_id_type=pl.DeviceIdType.MESH,
        )

    keep = pltpu.make_async_copy(stats_ref, got.at[me], send_sem.at[0])
    keep.start()

    @pl.loop(1, n_dev)
    def _(k):
        copy(k, me).start()

    @pl.loop(1, n_dev)
    def _(k):
        copy(k, lax.rem(me + n_dev - k, n_dev)).wait_recv()

    @pl.loop(1, n_dev)
    def _(k):
        copy(k, me).wait_send()

    keep.wait()
    top = got[0, 0]
    target = got[0, 1]
    for k in range(1, n_dev):
        top = jnp.maximum(top, got[k, 0])
        target = target + got[k, 1]
    total = jnp.zeros_like(top)
    for k in range(n_dev):
        total = total + jnp.exp(got[k, 0] - top)
    token_lp = target - (top + jnp.log(total))
    seqs, width = token_lp.shape
    row = lax.broadcasted_iota(jnp.int32, (seqs, width), 0)
    lane = lax.broadcasted_iota(jnp.int32, (seqs, width), 1)
    mine = row == lax.axis_index("tok")
    own_ref[...] = jnp.sum(jnp.where(mine, token_lp, 0.0), axis=0, keepdims=True)
    prompt = prompt_ref[...]
    reply = jnp.sum(jnp.where(lane >= prompt, token_lp, 0.0), axis=1, keepdims=True)
    advantage = reply / (width - prompt[:, :1]).astype(jnp.float32) - ref_ref[:, :1]
    slot = slot_ref[...]
    chosen = lax.bitwise_and(slot, 1) == 0
    signed = jnp.where(chosen, advantage, -advantage)
    pair = lax.shift_right_logical(slot, 1)
    margins = beta_scale * jnp.sum(jnp.where(pair == lane, signed, 0.0), axis=0, keepdims=True)
    margin_ref[...] = margins
    softplus = jnp.maximum(-margins, 0.0) + jnp.log1p(jnp.exp(-jnp.abs(margins)))
    n_pairs = seqs // 2
    loss = jnp.sum(jnp.where(lane[:1] < n_pairs, softplus, 0.0), axis=1, keepdims=True) / n_pairs
    loss_ref[...] = jnp.broadcast_to(loss, loss_ref.shape)


def exchange_and_finish(stats, slot, prompt_len, ref_means):
    n_tok = lax.axis_size("tok")
    n_dev = n_tok * lax.axis_size("voc")
    seqs, width = stats.shape[1:]
    wide = lambda v: jnp.broadcast_to(v[:, None], (seqs, width))
    row = jax.ShapeDtypeStruct((1, width), jnp.float32)
    own, margins, loss = pl.pallas_call(
        functools.partial(finish_kernel, n_tok, n_dev),
        out_shape=(row, row, row),
        in_specs=[pl.BlockSpec(memory_space=pltpu.VMEM)] * 4,
        out_specs=(pl.BlockSpec(memory_space=pltpu.VMEM),) * 3,
        scratch_shapes=[
            pltpu.VMEM((n_dev,) + stats.shape, jnp.float32),
            pltpu.SemaphoreType.DMA((n_dev,)),
            pltpu.SemaphoreType.DMA((n_dev,)),
        ],
        compiler_params=pltpu.CompilerParams(collective_id=1, has_side_effects=True),
    )(stats, wide(slot), wide(prompt_len), wide(ref_means))
    return own.reshape(-1), margins[0, : seqs // 2], loss[0, 0]


def gather_kernel(n_tok, hidden_ref, full_ref, local_sem, send_sem, recv_sem):
    tok, voc = lax.axis_index("tok"), lax.axis_index("voc")
    rows, width = hidden_ref.shape
    half = rows // 2
    n_z = n_tok // 2
    z, y = tok // 2, tok % 2
    other_y = tok + 1 - 2 * y
    other_x = (voc + 2) % 4
    sibling = voc + 1 - 2 * (voc % 2)
    to_x = {"tok": tok, "voc": other_x}
    to_y = {"tok": other_y, "voc": voc}
    to_sibling = {"tok": tok, "voc": sibling}

    def tok_at(offset, row):
        return ((z + offset) % n_z) * 2 + row

    barrier = pltpu.get_barrier_semaphore()
    for offset in range(1, n_z):
        pl.semaphore_signal(barrier, inc=1, device_id={"tok": tok_at(offset, y), "voc": voc}, device_id_type=pl.DeviceIdType.MESH)
    for peer in (to_x, to_y, to_sibling):
        pl.semaphore_signal(barrier, inc=1, device_id=peer, device_id_type=pl.DeviceIdType.MESH)
    pl.semaphore_wait(barrier, n_z + 2)

    def place(t, v, first=0, count=rows):
        return full_ref.at[pl.ds(pl.multiple_of(t * rows + first, 32), count), pl.ds(pl.multiple_of(v * width, LANES), width)]

    Z, X, Y, XH, YH, SZ, SX, SY, SXH, SYH = range(10)
    sent = []

    def send(kind, offset, source, target, device):
        index = kind * n_z + offset
        copy = pltpu.make_async_remote_copy(
            src_ref=source,
            dst_ref=target,
            send_sem=send_sem.at[index],
            recv_sem=recv_sem.at[index],
            device_id=device,
            device_id_type=pl.DeviceIdType.MESH,
        )
        copy.start()
        sent.append(copy)

    def arrived(kind, offset, target):
        index = kind * n_z + offset
        pltpu.make_async_remote_copy(
            src_ref=target,
            dst_ref=target,
            send_sem=send_sem.at[index],
            recv_sem=recv_sem.at[index],
            device_id=to_sibling,
            device_id_type=pl.DeviceIdType.MESH,
        ).wait_recv()

    own = place(tok, voc)
    for offset in sorted(range(1, n_z), key=lambda o: min(o, n_z - o)):
        send(Z, offset, hidden_ref, own, {"tok": tok_at(n_z - offset, y), "voc": voc})

    def spread(offset, source):
        here = place(tok_at(offset, y), voc)
        send(X, offset, source, here, to_x)
        send(Y, offset, source, here, to_y)
        send(SZ, offset, source, here, to_sibling)

    def forward(offset):
        across_x = (tok_at(offset, y), other_x)
        arrived(X, offset, place(*across_x))
        part = place(*across_x, 0, half)
        send(YH, offset, part, part, to_y)
        send(SX, offset, place(*across_x), place(*across_x), to_sibling)
        across_y = (tok_at(offset, 1 - y), voc)
        arrived(Y, offset, place(*across_y))
        part = place(*across_y, half, half)
        send(XH, offset, part, part, to_x)
        send(SY, offset, place(*across_y), place(*across_y), to_sibling)

    def finish(offset):
        corner = (tok_at(offset, 1 - y), other_x)
        for kind, sib, first in ((YH, SYH, 0), (XH, SXH, half)):
            part = place(*corner, first, half)
            arrived(kind, offset, part)
            send(sib, offset, part, part, to_sibling)

    order = sorted(range(n_z), key=lambda o: min(o, n_z - o))
    for i in range(n_z + 2):
        if i == 0:
            spread(0, hidden_ref)
            keep = pltpu.make_async_copy(hidden_ref, own, local_sem)
            keep.start()
        elif i < n_z:
            here = place(tok_at(order[i], y), voc)
            arrived(Z, order[i], here)
            spread(order[i], here)
        if 1 <= i <= n_z:
            forward(order[i - 1])
        if i >= 2:
            finish(order[i - 2])
    far_x = other_x + 1 - 2 * (other_x % 2)
    for o in range(n_z):
        arrived(SZ, o, place(tok_at(o, y), sibling))
        arrived(SX, o, place(tok_at(o, y), far_x))
        arrived(SY, o, place(tok_at(o, 1 - y), sibling))
        arrived(SYH, o, place(tok_at(o, 1 - y), far_x, 0, half))
        arrived(SXH, o, place(tok_at(o, 1 - y), far_x, half, half))
    keep.wait()
    for copy in sent:
        copy.wait_send()


def gather_hidden(hidden):
    n_tok, n_voc = lax.axis_size("tok"), lax.axis_size("voc")
    rows, width = hidden.shape
    if n_voc != 4 or n_tok % 2 or width % LANES or rows % 64:
        all_rows = lax.all_gather(hidden, "tok", axis=0, tiled=True)
        return lax.all_gather(all_rows, "voc", axis=1, tiled=True)
    copies = 10 * (n_tok // 2)
    return pl.pallas_call(
        functools.partial(gather_kernel, n_tok),
        out_shape=jax.ShapeDtypeStruct((rows * n_tok, width * n_voc), hidden.dtype),
        in_specs=[pl.BlockSpec(memory_space=pl.ANY)],
        out_specs=pl.BlockSpec(memory_space=pl.ANY),
        scratch_shapes=[
            pltpu.SemaphoreType.DMA,
            pltpu.SemaphoreType.DMA((copies,)),
            pltpu.SemaphoreType.DMA((copies,)),
        ],
        compiler_params=pltpu.CompilerParams(collective_id=2, has_side_effects=True),
    )(hidden)


def plan_rows(cols):
    fits = [t for t in range(16, 801, 16) if cols % (2 * t) == 0]
    return fits[-1] if fits else 0


def fold_tile(x_ref, wanted, base, m_ref, s_ref, t_ref):
    rows, width = x_ref.shape
    lanes = 4
    sub = lax.broadcasted_iota(jnp.int32, (SUBS, LANES), 0)
    for c in range(width // LANES):
        at = slice(c * LANES, (c + 1) * LANES)
        m_old = m_ref[:, at]
        tops = [m_old] + [jnp.full_like(m_old, LOW)] * (lanes - 1)
        for i in range(rows // SUBS):
            tops[i % lanes] = jnp.maximum(tops[i % lanes], x_ref[i * SUBS : (i + 1) * SUBS, at])
        m_new = functools.reduce(jnp.maximum, tops)
        sums = [s_ref[:, at] * jnp.exp(m_old - m_new)] + [jnp.zeros_like(m_old)] * (lanes - 1)
        hits = [t_ref[:, at]] + [jnp.zeros_like(m_old)] * (lanes - 1)
        want = wanted[c] - base - sub
        for i in range(rows // SUBS):
            x = x_ref[i * SUBS : (i + 1) * SUBS, at]
            sums[i % lanes] = sums[i % lanes] + jnp.exp(x - m_new)
            hits[i % lanes] = hits[i % lanes] + jnp.where(want == i * SUBS, x, 0.0)
        m_ref[:, at] = m_new
        s_ref[:, at] = functools.reduce(jnp.add, sums)
        t_ref[:, at] = functools.reduce(jnp.add, hits)


def fused_kernel(
    n_tok, n_dev, tile,
    hidden_ref, weight_ref, tgt_ref, slot_ref, prompt_ref, ref_ref, out_ref,
    full_ref, ring_ref, a_ref, b_ref, m_ref, s_ref, t_ref, got_ref, lp_ref,
    ring_sem, local_sem, send_sem, recv_sem, stat_send, stat_recv,
):
    tok, voc = lax.axis_index("tok"), lax.axis_index("voc")
    me = voc * n_tok + tok
    rows, width = hidden_ref.shape
    cols = weight_ref.shape[0]
    half = rows // 2
    n_z = n_tok // 2
    z, y = tok // 2, tok % 2
    other_y = tok + 1 - 2 * y
    other_x = (voc + 2) % 4
    sibling = voc + 1 - 2 * (voc % 2)
    far_x = other_x + 1 - 2 * (other_x % 2)
    to_x = {"tok": tok, "voc": other_x}
    to_y = {"tok": other_y, "voc": voc}
    to_sibling = {"tok": tok, "voc": sibling}

    pairs = cols // (2 * tile)
    slots = ring_ref.shape[0]
    sweeps = 3

    def load(n, part):
        start = pl.multiple_of((lax.rem(n, pairs) * 2 + part) * tile, 16)
        return pltpu.make_async_copy(
            weight_ref.at[pl.ds(start, tile)],
            ring_ref.at[lax.rem(n, slots), pl.ds(part * tile, tile)],
            ring_sem.at[lax.rem(n, slots), part],
        )

    def place(o, t, v, first=0, count=rows):
        return full_ref.at[pl.ds(pl.multiple_of((2 * o + t) * rows + first, 32), count), pl.ds(pl.multiple_of(v * width, LANES), width)]

    keep = pltpu.make_async_copy(hidden_ref, place(0, y, voc), local_sem)
    keep.start()
    for n in range(slots):
        for part in range(2):
            load(n, part).start()

    def peer(k):
        other = lax.rem(me + k, n_dev)
        return {"tok": lax.rem(other, n_tok), "voc": lax.div(other, n_tok)}

    barrier = pltpu.get_barrier_semaphore()

    @pl.loop(1, n_dev)
    def _(k):
        pl.semaphore_signal(barrier, inc=1, device_id=peer(k), device_id_type=pl.DeviceIdType.MESH)

    keep.wait()
    pl.semaphore_wait(barrier, n_dev - 1)

    Z, X, Y, XH, YH, SZ, SX, SY, SXH, SYH = range(10)
    sent = []

    def copy(kind, o):
        t, v, first, count, device = {
            Z: (y, voc, 0, rows, {"tok": ((z + n_z - o) % n_z) * 2 + y, "voc": voc}),
            X: (y, voc, 0, rows, to_x),
            Y: (y, voc, 0, rows, to_y),
            SZ: (y, voc, 0, rows, to_sibling),
            YH: (y, other_x, 0, half, to_y),
            SX: (y, other_x, 0, rows, to_sibling),
            XH: (1 - y, voc, half, half, to_x),
            SY: (1 - y, voc, 0, rows, to_sibling),
            SYH: (1 - y, other_x, 0, half, to_sibling),
            SXH: (1 - y, other_x, half, half, to_sibling),
        }[kind]
        source = place(0 if kind == Z else o, t, v, first, count)
        return pltpu.make_async_remote_copy(
            src_ref=source,
            dst_ref=place(o, t, v, first, count),
            send_sem=send_sem.at[kind * n_z + o],
            recv_sem=recv_sem.at[kind * n_z + o],
            device_id=device,
            device_id_type=pl.DeviceIdType.MESH,
        )

    def send(kind, o):
        copy(kind, o).start()
        sent.append((kind, o))

    def arrived(kind, o):
        t, v, first, count = {
            Z: (y, voc, 0, rows),
            X: (y, other_x, 0, rows),
            Y: (1 - y, voc, 0, rows),
            SZ: (y, sibling, 0, rows),
            YH: (1 - y, other_x, 0, half),
            SX: (y, far_x, 0, rows),
            XH: (1 - y, other_x, half, half),
            SY: (1 - y, sibling, 0, rows),
            SYH: (1 - y, far_x, 0, half),
            SXH: (1 - y, far_x, half, half),
        }[kind]
        target = place(o, t, v, first, count)
        pltpu.make_async_remote_copy(
            src_ref=target,
            dst_ref=target,
            send_sem=send_sem.at[kind * n_z + o],
            recv_sem=recv_sem.at[kind * n_z + o],
            device_id=to_sibling,
            device_id_type=pl.DeviceIdType.MESH,
        ).wait_recv()

    def spread(o):
        if o:
            arrived(Z, o)
        for kind in (X, Y, SZ):
            send(kind, o)

    def forward(o):
        arrived(X, o)
        send(YH, o)
        send(SX, o)
        arrived(Y, o)
        send(XH, o)
        send(SY, o)

    def finish(o):
        arrived(YH, o)
        send(SYH, o)
        arrived(XH, o)
        send(SXH, o)

    def settle(o):
        for kind in (SZ, SX, SY, SYH, SXH):
            arrived(kind, o)

    def stat_copy(k, source, piece):
        part = got_ref.at[source, pl.ds(piece * 2, 2)]
        return pltpu.make_async_remote_copy(
            src_ref=part,
            dst_ref=part,
            send_sem=stat_send.at[piece, k],
            recv_sem=stat_recv.at[piece, k],
            device_id=peer(k),
            device_id_type=pl.DeviceIdType.MESH,
        )

    def tell(piece):
        @pl.loop(1, n_dev)
        def _(k):
            stat_copy(k, me, piece).start()

    spread(0)
    for o in (1, 3, 2):
        send(Z, o)
    forward(0)
    finish(0)
    settle(0)

    col_start = me * cols

    def sweep(turn, first, planes, actions):
        size = planes * 2 * rows
        wanted = []
        for o in range(first, first + planes):
            for t in range(2):
                local = tgt_ref[pl.ds(((z + o) % n_z) * 2 + t, 1), :] - col_start
                wanted.append(jnp.where((local >= 0) & (local < cols), local, -(1 << 30)))
        x_a, x_b = a_ref.at[:, pl.ds(0, size)], b_ref.at[:, pl.ds(0, size)]
        m, s, t = (r.at[:, pl.ds(0, size)] for r in (m_ref, s_ref, t_ref))
        x_b[...] = jnp.full_like(x_b, LOW)
        m[...] = jnp.full_like(m, LOW)
        s[...] = jnp.zeros_like(s)
        t[...] = jnp.zeros_like(t)

        def step(i, carry):
            n = turn * pairs + i
            for at, action in actions:
                pl.when(i == at)(action)
            for part in range(2):
                load(n, part).wait()

            @pl.when((n >= 1) & (n - 1 + slots < sweeps * pairs))
            def _():
                for part in range(2):
                    load(n - 1 + slots, part).start()

            slot = lax.rem(n, slots)
            h = lambda: full_ref[first * 2 * rows : first * 2 * rows + size, :]
            base = i * (2 * tile)
            x_a[...] = lax.dot_general(ring_ref[slot, :tile, :], h(), NT, preferred_element_type=jnp.float32)
            fold_tile(x_b, wanted, base - tile, m, s, t)
            x_b[...] = lax.dot_general(ring_ref[slot, tile:, :], h(), NT, preferred_element_type=jnp.float32)
            fold_tile(x_a, wanted, base, m, s, t)
            return carry

        lax.fori_loop(0, pairs, step, 0)
        fold_tile(x_b, wanted, cols - tile, m, s, t)
        high = m[...]
        top = jnp.max(high, axis=0, keepdims=True)
        total = jnp.sum(s[...] * jnp.exp(high - top), axis=0, keepdims=True)
        lse = top + jnp.log(total)
        hit = jnp.sum(t[...], axis=0, keepdims=True)
        for p in range(planes):
            for q in range(2):
                at = slice((2 * p + q) * LANES, (2 * p + q + 1) * LANES)
                got_ref[me, first + p, q : q + 1, :] = lse[:, at]
                got_ref[me, first + p, 2 + q : 3 + q, :] = hit[:, at]

    def act(*calls):
        def run():
            for call, o in calls:
                call(o)

        return run

    sweep(0, 0, 1, [(0, act((spread, 1))), (2, act((forward, 1), (spread, 3))), (4, act((finish, 1), (forward, 3), (spread, 2)))])
    settle(1)
    sweep(1, 1, 1, [(1, act((finish, 3), (forward, 2))), (3, act((finish, 2)))])
    settle(3)
    settle(2)
    sweep(2, 2, 2, [(1, act((tell, 0)))])
    tell(1)
    for kind, o in sent:
        copy(kind, o).wait_send()

    @pl.loop(1, n_dev)
    def _(k):
        for piece in range(2):
            stat_copy(k, lax.rem(me + n_dev - k, n_dev), piece).wait_recv()

    @pl.loop(1, n_dev)
    def _(k):
        for piece in range(2):
            stat_copy(k, me, piece).wait_send()

    for g in range(n_z):
        of = lambda k: got_ref[k, (g - (k % n_tok) // 2) % n_z]
        top = functools.reduce(jnp.maximum, [of(k)[:2] for k in range(n_dev)])
        total = functools.reduce(jnp.add, [jnp.exp(of(k)[:2] - top) for k in range(n_dev)])
        hit = functools.reduce(jnp.add, [of(k)[2:] for k in range(n_dev)])
        lp_ref[2 * g : 2 * g + 2, :] = hit - (top + jnp.log(total))
    token_lp = lp_ref[...]
    seqs, length = token_lp.shape
    row = lax.broadcasted_iota(jnp.int32, (seqs, length), 0)
    lane = lax.broadcasted_iota(jnp.int32, (seqs, length), 1)
    spread_out = lambda ref: functools.reduce(lambda v, q: jnp.where(row == q, ref[q], v), range(1, seqs), jnp.full(row.shape, ref[0]))
    prompt, slot, ref_mean = spread_out(prompt_ref), spread_out(slot_ref), spread_out(ref_ref)
    own = jnp.sum(jnp.where(row == tok, token_lp, 0.0), axis=0, keepdims=True)
    reply = jnp.sum(jnp.where(lane >= prompt, token_lp, 0.0), axis=1, keepdims=True)
    advantage = reply / (length - prompt).astype(jnp.float32) - ref_mean
    signed = jnp.where(lax.bitwise_and(slot, 1) == 0, advantage, -advantage)
    pair = lax.shift_right_logical(slot, 1)
    margins = beta_scale * jnp.sum(jnp.where(pair == lane, signed, 0.0), axis=0, keepdims=True)
    softplus = jnp.maximum(-margins, 0.0) + jnp.log1p(jnp.exp(-jnp.abs(margins)))
    n_pairs = seqs // 2
    loss = jnp.sum(jnp.where(lane[:1] < n_pairs, softplus, 0.0), axis=1, keepdims=True) / n_pairs
    out_ref[0:1, :] = own
    out_ref[1:2, :] = margins
    out_ref[2:3, :] = jnp.broadcast_to(loss, margins.shape)


def fused(hidden, weight, targets, slot, prompt_len, ref_means):
    n_tok = lax.axis_size("tok")
    n_dev = n_tok * lax.axis_size("voc")
    rows = hidden.shape[0]
    cols, depth = weight.shape
    tile = plan_rows(cols)
    n_z = n_tok // 2
    whole = pl.BlockSpec(memory_space=pltpu.VMEM)
    wide = pl.BlockSpec(memory_space=pl.ANY)
    scalars = pl.BlockSpec(memory_space=pltpu.SMEM)
    ring = 4
    copies = 10 * n_z
    out = pl.pallas_call(
        functools.partial(fused_kernel, n_tok, n_dev, tile),
        out_shape=jax.ShapeDtypeStruct((3, rows), jnp.float32),
        in_specs=[wide, wide, whole, scalars, scalars, scalars],
        out_specs=whole,
        scratch_shapes=[
            pltpu.VMEM((rows * n_tok, depth), hidden.dtype),
            pltpu.VMEM((ring, 2 * tile, depth), weight.dtype),
            pltpu.VMEM((tile, 4 * rows), jnp.float32),
            pltpu.VMEM((tile, 4 * rows), jnp.float32),
            pltpu.VMEM((SUBS, 4 * rows), jnp.float32),
            pltpu.VMEM((SUBS, 4 * rows), jnp.float32),
            pltpu.VMEM((SUBS, 4 * rows), jnp.float32),
            pltpu.VMEM((n_dev, n_z, 4, rows), jnp.float32),
            pltpu.VMEM((n_tok, rows), jnp.float32),
            pltpu.SemaphoreType.DMA((ring, 2)),
            pltpu.SemaphoreType.DMA,
            pltpu.SemaphoreType.DMA((copies,)),
            pltpu.SemaphoreType.DMA((copies,)),
            pltpu.SemaphoreType.DMA((2, n_dev)),
            pltpu.SemaphoreType.DMA((2, n_dev)),
        ],
        compiler_params=pltpu.CompilerParams(collective_id=3, has_side_effects=True, vmem_limit_bytes=63 * 1024 * 1024),
        cost_estimate=pl.CostEstimate(flops=2 * rows * n_tok * depth * cols, bytes_accessed=6 * depth * cols, transcendentals=rows * n_tok * cols),
    )(hidden, weight, targets.reshape(n_tok, rows), slot, prompt_len, ref_means)
    return out[0], out[1, : n_tok // 2], out[2, 0]


def body(hidden, weight, targets, slot, prompt_len, ref_means):
    vocab_cols = weight.shape[1]
    n_tok = lax.axis_size("tok")
    rows, width = hidden.shape
    if lax.axis_size("voc") == 4 and n_tok == 8 and width % LANES == 0 and rows == LANES and vocab_cols >= 10 * plan_rows(vocab_cols) > 0:
        return fused(hidden, weight.T, targets, slot, prompt_len, ref_means)
    col_start = (lax.axis_index("voc") * lax.axis_size("tok") + lax.axis_index("tok")) * vocab_cols
    local = targets - col_start
    local = jnp.where((local >= 0) & (local < vocab_cols), local, -(1 << 30))
    wanted = jnp.broadcast_to(local[:, None], (targets.shape[0], LANES))
    stats = local_stats(gather_hidden(hidden), weight.T, wanted)
    return exchange_and_finish(stats, slot, prompt_len, ref_means)


def solution(mesh):
    in_specs = (P("tok", "voc"), P(None, ("voc", "tok")), P(), P(), P(), P())
    out_specs = (P("tok"), P(), P())
    return jax.shard_map(body, mesh=mesh, in_specs=in_specs, out_specs=out_specs, check_vma=False)
```

```python
import functools

import jax
import jax.numpy as jnp
from jax import lax
from jax.experimental import pallas as pl
from jax.experimental.pallas import tpu as pltpu
from jax.sharding import PartitionSpec as P

beta_scale = 2.0
LOW = -1e30
LANES = 128
SUBS = 8
TILE = 512
CHUNK = 64
NT = (((1,), (1,)), ((), ()))


def stats_pass(x_ref, tgt_ref, m_ref, s_ref, t_ref, base, cols):
    lane = lax.broadcasted_iota(jnp.int32, (CHUNK, LANES), 1)
    for r in range(0, x_ref.shape[0], CHUNK):
        rows = pl.ds(r, CHUNK)
        wanted = tgt_ref[rows, :] - base
        xs = []
        for k in range(TILE // LANES):
            x = x_ref[rows, k * LANES : (k + 1) * LANES]
            xs.append(jnp.where(lane < cols - base - k * LANES, x, LOW))
        m_old = m_ref[rows, :]
        m_new = functools.reduce(jnp.maximum, xs, m_old)
        s = s_ref[rows, :] * jnp.exp(m_old - m_new)
        t = t_ref[rows, :]
        for k, x in enumerate(xs):
            s = s + jnp.exp(x - m_new)
            t = t + jnp.where(wanted == lane + k * LANES, x, 0.0)
        m_ref[rows, :] = m_new
        s_ref[rows, :] = s
        t_ref[rows, :] = t


def logits_kernel(cols, h_ref, w_ref, tgt_ref, out_ref, a_ref, b_ref, m_ref, s_ref, t_ref):
    step = pl.program_id(0)

    @pl.when(step == 0)
    def _():
        b_ref[...] = jnp.full_like(b_ref, LOW)
        m_ref[...] = jnp.full_like(m_ref, LOW)
        s_ref[...] = jnp.zeros_like(s_ref)
        t_ref[...] = jnp.zeros_like(t_ref)

    base = step * (2 * TILE)
    fold = functools.partial(stats_pass, tgt_ref=tgt_ref, m_ref=m_ref, s_ref=s_ref, t_ref=t_ref, cols=cols)
    a_ref[...] = lax.dot_general(h_ref[...], w_ref[:TILE], NT, preferred_element_type=jnp.float32)
    fold(b_ref, base=base - TILE)
    b_ref[...] = lax.dot_general(h_ref[...], w_ref[TILE:], NT, preferred_element_type=jnp.float32)
    fold(a_ref, base=base)

    @pl.when(step == pl.num_programs(0) - 1)
    def _():
        fold(b_ref, base=base + TILE)
        diagonal = lax.broadcasted_iota(jnp.int32, (LANES, LANES), 0) == lax.broadcasted_iota(jnp.int32, (LANES, LANES), 1)
        for q in range(out_ref.shape[1]):
            rows = pl.ds(q * LANES, LANES)
            m = m_ref[rows, :]
            top = jnp.max(m, axis=1, keepdims=True)
            total = jnp.sum(s_ref[rows, :] * jnp.exp(m - top), axis=1, keepdims=True)
            lse = top + jnp.log(total)
            hit = jnp.sum(t_ref[rows, :], axis=1, keepdims=True)
            out_ref[0, pl.ds(q, 1), :] = jnp.sum(jnp.where(diagonal, lse, 0.0), axis=0, keepdims=True)
            out_ref[1, pl.ds(q, 1), :] = jnp.sum(jnp.where(diagonal, hit, 0.0), axis=0, keepdims=True)


def local_stats(full, weight, wanted):
    rows, depth = full.shape
    cols = weight.shape[0]
    steps = pl.cdiv(cols, 2 * TILE)
    whole = lambda i: (0, 0)
    return pl.pallas_call(
        functools.partial(logits_kernel, cols),
        grid=(steps,),
        out_shape=jax.ShapeDtypeStruct((2, rows // LANES, LANES), jnp.float32),
        in_specs=[
            pl.BlockSpec((rows, depth), whole),
            pl.BlockSpec((2 * TILE, depth), lambda i: (i, 0)),
            pl.BlockSpec((rows, LANES), whole),
        ],
        out_specs=pl.BlockSpec((2, rows // LANES, LANES), lambda i: (0, 0, 0)),
        scratch_shapes=[pltpu.VMEM((rows, TILE), jnp.float32)] * 2 + [pltpu.VMEM((rows, LANES), jnp.float32)] * 3,
        compiler_params=pltpu.CompilerParams(vmem_limit_bytes=62 * 1024 * 1024, dimension_semantics=("arbitrary",)),
        cost_estimate=pl.CostEstimate(flops=2 * rows * depth * cols, bytes_accessed=2 * depth * (rows + cols), transcendentals=rows * cols),
    )(full, weight, wanted)


def finish_kernel(n_tok, n_dev, stats_ref, slot_ref, prompt_ref, ref_ref, own_ref, margin_ref, loss_ref, got, send_sem, recv_sem):
    me = lax.axis_index("voc") * n_tok + lax.axis_index("tok")

    def peer(k):
        other = lax.rem(me + k, n_dev)
        return {"tok": lax.rem(other, n_tok), "voc": lax.div(other, n_tok)}

    barrier = pltpu.get_barrier_semaphore()

    @pl.loop(1, n_dev)
    def _(k):
        pl.semaphore_signal(barrier, inc=1, device_id=peer(k), device_id_type=pl.DeviceIdType.MESH)

    pl.semaphore_wait(barrier, n_dev - 1)

    def copy(k, source):
        return pltpu.make_async_remote_copy(
            src_ref=stats_ref,
            dst_ref=got.at[source],
            send_sem=send_sem.at[k],
            recv_sem=recv_sem.at[k],
            device_id=peer(k),
            device_id_type=pl.DeviceIdType.MESH,
        )

    keep = pltpu.make_async_copy(stats_ref, got.at[me], send_sem.at[0])
    keep.start()

    @pl.loop(1, n_dev)
    def _(k):
        copy(k, me).start()

    @pl.loop(1, n_dev)
    def _(k):
        copy(k, lax.rem(me + n_dev - k, n_dev)).wait_recv()

    @pl.loop(1, n_dev)
    def _(k):
        copy(k, me).wait_send()

    keep.wait()
    top = got[0, 0]
    target = got[0, 1]
    for k in range(1, n_dev):
        top = jnp.maximum(top, got[k, 0])
        target = target + got[k, 1]
    total = jnp.zeros_like(top)
    for k in range(n_dev):
        total = total + jnp.exp(got[k, 0] - top)
    token_lp = target - (top + jnp.log(total))
    seqs, width = token_lp.shape
    row = lax.broadcasted_iota(jnp.int32, (seqs, width), 0)
    lane = lax.broadcasted_iota(jnp.int32, (seqs, width), 1)
    mine = row == lax.axis_index("tok")
    own_ref[...] = jnp.sum(jnp.where(mine, token_lp, 0.0), axis=0, keepdims=True)
    prompt = prompt_ref[...]
    reply = jnp.sum(jnp.where(lane >= prompt, token_lp, 0.0), axis=1, keepdims=True)
    advantage = reply / (width - prompt[:, :1]).astype(jnp.float32) - ref_ref[:, :1]
    slot = slot_ref[...]
    chosen = lax.bitwise_and(slot, 1) == 0
    signed = jnp.where(chosen, advantage, -advantage)
    pair = lax.shift_right_logical(slot, 1)
    margins = beta_scale * jnp.sum(jnp.where(pair == lane, signed, 0.0), axis=0, keepdims=True)
    margin_ref[...] = margins
    softplus = jnp.maximum(-margins, 0.0) + jnp.log1p(jnp.exp(-jnp.abs(margins)))
    n_pairs = seqs // 2
    loss = jnp.sum(jnp.where(lane[:1] < n_pairs, softplus, 0.0), axis=1, keepdims=True) / n_pairs
    loss_ref[...] = jnp.broadcast_to(loss, loss_ref.shape)


def exchange_and_finish(stats, slot, prompt_len, ref_means):
    n_tok = lax.axis_size("tok")
    n_dev = n_tok * lax.axis_size("voc")
    seqs, width = stats.shape[1:]
    wide = lambda v: jnp.broadcast_to(v[:, None], (seqs, width))
    row = jax.ShapeDtypeStruct((1, width), jnp.float32)
    own, margins, loss = pl.pallas_call(
        functools.partial(finish_kernel, n_tok, n_dev),
        out_shape=(row, row, row),
        in_specs=[pl.BlockSpec(memory_space=pltpu.VMEM)] * 4,
        out_specs=(pl.BlockSpec(memory_space=pltpu.VMEM),) * 3,
        scratch_shapes=[
            pltpu.VMEM((n_dev,) + stats.shape, jnp.float32),
            pltpu.SemaphoreType.DMA((n_dev,)),
            pltpu.SemaphoreType.DMA((n_dev,)),
        ],
        compiler_params=pltpu.CompilerParams(collective_id=1, has_side_effects=True),
    )(stats, wide(slot), wide(prompt_len), wide(ref_means))
    return own.reshape(-1), margins[0, : seqs // 2], loss[0, 0]


def gather_kernel(n_tok, hidden_ref, full_ref, local_sem, send_sem, recv_sem):
    tok, voc = lax.axis_index("tok"), lax.axis_index("voc")
    rows, width = hidden_ref.shape
    half = rows // 2
    n_z = n_tok // 2
    z, y = tok // 2, tok % 2
    other_y = tok + 1 - 2 * y
    other_x = (voc + 2) % 4
    sibling = voc + 1 - 2 * (voc % 2)
    to_x = {"tok": tok, "voc": other_x}
    to_y = {"tok": other_y, "voc": voc}
    to_sibling = {"tok": tok, "voc": sibling}

    def tok_at(offset, row):
        return ((z + offset) % n_z) * 2 + row

    barrier = pltpu.get_barrier_semaphore()
    for offset in range(1, n_z):
        pl.semaphore_signal(barrier, inc=1, device_id={"tok": tok_at(offset, y), "voc": voc}, device_id_type=pl.DeviceIdType.MESH)
    for peer in (to_x, to_y, to_sibling):
        pl.semaphore_signal(barrier, inc=1, device_id=peer, device_id_type=pl.DeviceIdType.MESH)
    pl.semaphore_wait(barrier, n_z + 2)

    def place(t, v, first=0, count=rows):
        return full_ref.at[pl.ds(pl.multiple_of(t * rows + first, 32), count), pl.ds(pl.multiple_of(v * width, LANES), width)]

    Z, X, Y, XH, YH, SZ, SX, SY, SXH, SYH = range(10)
    sent = []

    def send(kind, offset, source, target, device):
        index = kind * n_z + offset
        copy = pltpu.make_async_remote_copy(
            src_ref=source,
            dst_ref=target,
            send_sem=send_sem.at[index],
            recv_sem=recv_sem.at[index],
            device_id=device,
            device_id_type=pl.DeviceIdType.MESH,
        )
        copy.start()
        sent.append(copy)

    def arrived(kind, offset, target):
        index = kind * n_z + offset
        pltpu.make_async_remote_copy(
            src_ref=target,
            dst_ref=target,
            send_sem=send_sem.at[index],
            recv_sem=recv_sem.at[index],
            device_id=to_sibling,
            device_id_type=pl.DeviceIdType.MESH,
        ).wait_recv()

    own = place(tok, voc)
    for offset in sorted(range(1, n_z), key=lambda o: min(o, n_z - o)):
        send(Z, offset, hidden_ref, own, {"tok": tok_at(n_z - offset, y), "voc": voc})

    def spread(offset, source):
        here = place(tok_at(offset, y), voc)
        send(X, offset, source, here, to_x)
        send(Y, offset, source, here, to_y)
        send(SZ, offset, source, here, to_sibling)

    def forward(offset):
        across_x = (tok_at(offset, y), other_x)
        arrived(X, offset, place(*across_x))
        part = place(*across_x, 0, half)
        send(YH, offset, part, part, to_y)
        send(SX, offset, place(*across_x), place(*across_x), to_sibling)
        across_y = (tok_at(offset, 1 - y), voc)
        arrived(Y, offset, place(*across_y))
        part = place(*across_y, half, half)
        send(XH, offset, part, part, to_x)
        send(SY, offset, place(*across_y), place(*across_y), to_sibling)

    def finish(offset):
        corner = (tok_at(offset, 1 - y), other_x)
        for kind, sib, first in ((YH, SYH, 0), (XH, SXH, half)):
            part = place(*corner, first, half)
            arrived(kind, offset, part)
            send(sib, offset, part, part, to_sibling)

    order = sorted(range(n_z), key=lambda o: min(o, n_z - o))
    for i in range(n_z + 2):
        if i == 0:
            spread(0, hidden_ref)
            keep = pltpu.make_async_copy(hidden_ref, own, local_sem)
            keep.start()
        elif i < n_z:
            here = place(tok_at(order[i], y), voc)
            arrived(Z, order[i], here)
            spread(order[i], here)
        if 1 <= i <= n_z:
            forward(order[i - 1])
        if i >= 2:
            finish(order[i - 2])
    far_x = other_x + 1 - 2 * (other_x % 2)
    for o in range(n_z):
        arrived(SZ, o, place(tok_at(o, y), sibling))
        arrived(SX, o, place(tok_at(o, y), far_x))
        arrived(SY, o, place(tok_at(o, 1 - y), sibling))
        arrived(SYH, o, place(tok_at(o, 1 - y), far_x, 0, half))
        arrived(SXH, o, place(tok_at(o, 1 - y), far_x, half, half))
    keep.wait()
    for copy in sent:
        copy.wait_send()


def gather_hidden(hidden):
    n_tok, n_voc = lax.axis_size("tok"), lax.axis_size("voc")
    rows, width = hidden.shape
    if n_voc != 4 or n_tok % 2 or width % LANES or rows % 64:
        all_rows = lax.all_gather(hidden, "tok", axis=0, tiled=True)
        return lax.all_gather(all_rows, "voc", axis=1, tiled=True)
    copies = 10 * (n_tok // 2)
    return pl.pallas_call(
        functools.partial(gather_kernel, n_tok),
        out_shape=jax.ShapeDtypeStruct((rows * n_tok, width * n_voc), hidden.dtype),
        in_specs=[pl.BlockSpec(memory_space=pl.ANY)],
        out_specs=pl.BlockSpec(memory_space=pl.ANY),
        scratch_shapes=[
            pltpu.SemaphoreType.DMA,
            pltpu.SemaphoreType.DMA((copies,)),
            pltpu.SemaphoreType.DMA((copies,)),
        ],
        compiler_params=pltpu.CompilerParams(collective_id=2, has_side_effects=True),
    )(hidden)


def plan_rows(cols):
    fits = [t for t in range(16, 801, 16) if cols % (2 * t) == 0]
    return fits[-1] if fits else 0


def fold_tile(x_ref, wanted, base, m_ref, s_ref, t_ref):
    rows, width = x_ref.shape
    lanes = 4
    sub = lax.broadcasted_iota(jnp.int32, (SUBS, LANES), 0)
    for c in range(width // LANES):
        at = slice(c * LANES, (c + 1) * LANES)
        m_old = m_ref[:, at]
        tops = [m_old] + [jnp.full_like(m_old, LOW)] * (lanes - 1)
        for i in range(rows // SUBS):
            tops[i % lanes] = jnp.maximum(tops[i % lanes], x_ref[i * SUBS : (i + 1) * SUBS, at])
        m_new = functools.reduce(jnp.maximum, tops)
        sums = [s_ref[:, at] * jnp.exp(m_old - m_new)] + [jnp.zeros_like(m_old)] * (lanes - 1)
        hits = [t_ref[:, at]] + [jnp.zeros_like(m_old)] * (lanes - 1)
        want = wanted[c] - base - sub
        for i in range(rows // SUBS):
            x = x_ref[i * SUBS : (i + 1) * SUBS, at]
            sums[i % lanes] = sums[i % lanes] + jnp.exp(x - m_new)
            hits[i % lanes] = jnp.where(want == i * SUBS, x, hits[i % lanes])
        m_ref[:, at] = m_new
        s_ref[:, at] = functools.reduce(jnp.add, sums)
        t_ref[:, at] = functools.reduce(jnp.add, hits)


def fused_kernel(
    n_tok, n_dev, tile,
    hidden_ref, weight_ref, tgt_ref, slot_ref, prompt_ref, ref_ref, own_ref, margin_ref, loss_ref,
    full_ref, ring_ref, a_ref, b_ref, c_ref, m_ref, s_ref, t_ref, near_ref, got_ref, lp_ref,
    ring_sem, local_sem, send_sem, recv_sem, stat_send, stat_recv,
):
    tok, voc = lax.axis_index("tok"), lax.axis_index("voc")
    me = voc * n_tok + tok
    rows, width = hidden_ref.shape
    cols = weight_ref.shape[0]
    half = rows // 2
    n_z = n_tok // 2
    z, y = tok // 2, tok % 2
    other_y = tok + 1 - 2 * y
    other_x = (voc + 2) % 4
    sibling = voc + 1 - 2 * (voc % 2)
    far_x = other_x + 1 - 2 * (other_x % 2)
    to_x = {"tok": tok, "voc": other_x}
    to_y = {"tok": other_y, "voc": voc}
    to_sibling = {"tok": tok, "voc": sibling}

    pairs = cols // (2 * tile)
    slots = ring_ref.shape[0]
    sweeps = 3

    def load(n, part):
        start = pl.multiple_of((lax.rem(n, pairs) * 2 + part) * tile, 16)
        return pltpu.make_async_copy(
            weight_ref.at[pl.ds(start, tile)],
            ring_ref.at[lax.rem(n, slots), pl.ds(part * tile, tile)],
            ring_sem.at[lax.rem(n, slots), part],
        )

    def place(o, t, v, first=0, count=rows):
        return full_ref.at[pl.ds(pl.multiple_of((2 * o + t) * rows + first, 32), count), pl.ds(pl.multiple_of(v * width, LANES), width)]

    keep = pltpu.make_async_copy(hidden_ref, place(0, y, voc), local_sem)
    keep.start()
    for n in range(1):
        for part in range(2):
            load(n, part).start()

    n_voc = n_dev // n_tok
    peers = [{"tok": (tok + k) % n_tok, "voc": voc} for k in range(1, n_tok)]
    peers += [{"tok": tok, "voc": (voc + k) % n_voc} for k in range(1, n_voc)]
    barrier = pltpu.get_barrier_semaphore()
    for device in peers:
        pl.semaphore_signal(barrier, inc=1, device_id=device, device_id_type=pl.DeviceIdType.MESH)
    keep.wait()
    pl.semaphore_wait(barrier, len(peers))

    Z, X, Y, XH, YH, SZ, SX, SY, SXH, SYH, XL, YL = range(12)
    sent = []

    def copy(kind, o):
        t, v, first, count, device = {
            Z: (y, voc, 0, rows, {"tok": ((z + n_z - o) % n_z) * 2 + y, "voc": voc}),
            X: (y, voc, 0, half, to_x),
            XL: (y, voc, half, half, to_x),
            Y: (y, voc, half, half, to_y),
            YL: (y, voc, 0, half, to_y),
            SZ: (y, voc, 0, rows, to_sibling),
            YH: (y, other_x, 0, half, to_y),
            SX: (y, other_x, 0, rows, to_sibling),
            XH: (1 - y, voc, half, half, to_x),
            SY: (1 - y, voc, 0, rows, to_sibling),
            SYH: (1 - y, other_x, 0, half, to_sibling),
            SXH: (1 - y, other_x, half, half, to_sibling),
        }[kind]
        source = place(0 if kind == Z else o, t, v, first, count)
        return pltpu.make_async_remote_copy(
            src_ref=source,
            dst_ref=place(o, t, v, first, count),
            send_sem=send_sem.at[kind * n_z + o],
            recv_sem=recv_sem.at[kind * n_z + o],
            device_id=device,
            device_id_type=pl.DeviceIdType.MESH,
        )

    def send(kind, o):
        copy(kind, o).start()
        sent.append((kind, o))

    def arrived(kind, o):
        t, v, first, count = {
            Z: (y, voc, 0, rows),
            X: (y, other_x, 0, half),
            XL: (y, other_x, half, half),
            Y: (1 - y, voc, half, half),
            YL: (1 - y, voc, 0, half),
            SZ: (y, sibling, 0, rows),
            YH: (1 - y, other_x, 0, half),
            SX: (y, far_x, 0, rows),
            XH: (1 - y, other_x, half, half),
            SY: (1 - y, sibling, 0, rows),
            SYH: (1 - y, far_x, 0, half),
            SXH: (1 - y, far_x, half, half),
        }[kind]
        target = place(o, t, v, first, count)
        pltpu.make_async_remote_copy(
            src_ref=target,
            dst_ref=target,
            send_sem=send_sem.at[kind * n_z + o],
            recv_sem=recv_sem.at[kind * n_z + o],
            device_id=to_sibling,
            device_id_type=pl.DeviceIdType.MESH,
        ).wait_recv()

    def spread(o):
        if o:
            arrived(Z, o)
        for kind in (X, Y, XL, YL, SZ):
            send(kind, o)

    def forward(o):
        arrived(X, o)
        send(YH, o)
        arrived(Y, o)
        send(XH, o)
        arrived(XL, o)
        send(SX, o)
        arrived(YL, o)
        send(SY, o)

    def finish(o):
        arrived(YH, o)
        send(SYH, o)
        arrived(XH, o)
        send(SXH, o)

    def settle(o):
        for kind in (SZ, SX, SY, SYH, SXH):
            arrived(kind, o)

    def exchange(box, mine, count, device_of, first):
        def stat(k, source):
            return pltpu.make_async_remote_copy(
                src_ref=box.at[source],
                dst_ref=box.at[source],
                send_sem=stat_send.at[first + k],
                recv_sem=stat_recv.at[first + k],
                device_id=device_of((mine + k) % count),
                device_id_type=pl.DeviceIdType.MESH,
            )

        for k in range(1, count):
            stat(k, mine).start()
        for k in range(1, count):
            stat(k, (mine + count - k) % count).wait_recv()
        return [stat(k, mine) for k in range(1, count)]

    spread(0)
    for o in (1, 3, 2):
        send(Z, o)
    forward(0)
    finish(0)
    settle(0)
    for n in range(1, slots):
        for part in range(2):
            load(n, part).start()

    col_start = me * cols

    def sweep(turn, first, planes, actions):
        size = planes * 2 * rows
        wanted = []
        for o in range(first, first + planes):
            for t in range(2):
                local = tgt_ref[pl.ds(((z + o) % n_z) * 2 + t, 1), :] - col_start
                wanted.append(jnp.where((local >= 0) & (local < cols), local, -(1 << 30)))
        blocks = ((a_ref, 0), (b_ref, tile)) if planes == 2 else ((c_ref, 0),)
        m, s, t = (r.at[:, pl.ds(0, size)] for r in (m_ref, s_ref, t_ref))
        for x, _ in blocks:
            x[...] = jnp.full_like(x, LOW)
        m[...] = jnp.full_like(m, LOW)
        s[...] = jnp.zeros_like(s)
        t[...] = jnp.zeros_like(t)

        def step(i, carry):
            n = turn * pairs + i
            for at, action in actions:
                pl.when(i == at)(action)
            for part in range(2):
                load(n, part).wait()

            @pl.when((n >= 1) & (n - 1 + slots < sweeps * pairs))
            def _():
                for part in range(2):
                    load(n - 1 + slots, part).start()

            slot = lax.rem(n, slots)
            h = lambda: full_ref[first * 2 * rows : first * 2 * rows + size, :]
            base = i * (2 * tile)
            for x, first_row in blocks:
                fold_tile(x, wanted, base + first_row - 2 * tile, m, s, t)
                w = ring_ref[slot, first_row : first_row + x.shape[0], :]
                x[...] = lax.dot_general(w, h(), NT, preferred_element_type=jnp.float32)
            return carry

        lax.fori_loop(0, pairs, step, 0)
        for x, first_row in blocks:
            fold_tile(x, wanted, cols + first_row - 2 * tile, m, s, t)
        high = m[...]
        top = jnp.max(high, axis=0, keepdims=True)
        total = jnp.sum(s[...] * jnp.exp(high - top), axis=0, keepdims=True)
        lse = top + jnp.log(total)
        hit = jnp.sum(t[...], axis=0, keepdims=True)
        for p in range(planes):
            for q in range(2):
                at = slice((2 * p + q) * LANES, (2 * p + q + 1) * LANES)
                near_ref[voc, first + p, q : q + 1, :] = lse[:, at]
                near_ref[voc, first + p, 2 + q : 3 + q, :] = hit[:, at]

    def act(*calls):
        def run():
            for call, o in calls:
                call(o)

        return run

    sweep(0, 0, 1, [(0, act((spread, 1))), (2, act((forward, 1), (spread, 3))), (4, act((finish, 1), (spread, 2)))])
    settle(1)
    sweep(1, 1, 1, [(0, act((forward, 3))), (2, act((finish, 3), (forward, 2))), (4, act((finish, 2)))])
    settle(3)
    settle(2)
    sweep(2, 2, 2, [])

    def merge(parts):
        top = functools.reduce(jnp.maximum, [p[:2] for p in parts])
        total = functools.reduce(jnp.add, [jnp.exp(p[:2] - top) for p in parts])
        return top + jnp.log(total), functools.reduce(jnp.add, [p[2:] for p in parts])

    pending = exchange(near_ref, voc, n_voc, lambda v: {"tok": tok, "voc": v}, 0)
    for o in range(n_z):
        lse, hit = merge([near_ref[v, o] for v in range(n_voc)])
        got_ref[tok, o, :2, :] = lse
        got_ref[tok, o, 2:, :] = hit
    pending += exchange(got_ref, tok, n_tok, lambda t: {"tok": t, "voc": voc}, n_voc)
    for kind, o in sent:
        copy(kind, o).wait_send()
    for stat in pending:
        stat.wait_send()
    for g in range(n_z):
        lse, hit = merge([got_ref[k, (g - k // 2) % n_z] for k in range(n_tok)])
        lp_ref[2 * g : 2 * g + 2, :] = hit - lse
    token_lp = lp_ref[...]
    seqs, length = token_lp.shape
    row = lax.broadcasted_iota(jnp.int32, (seqs, length), 0)
    lane = lax.broadcasted_iota(jnp.int32, (seqs, length), 1)
    spread_out = lambda ref: functools.reduce(lambda v, q: jnp.where(row == q, ref[q], v), range(1, seqs), jnp.full(row.shape, ref[0]))
    prompt, slot, ref_mean = spread_out(prompt_ref), spread_out(slot_ref), spread_out(ref_ref)
    own = jnp.sum(jnp.where(row == tok, token_lp, 0.0), axis=0, keepdims=True)
    reply = jnp.sum(jnp.where(lane >= prompt, token_lp, 0.0), axis=1, keepdims=True)
    advantage = reply / (length - prompt).astype(jnp.float32) - ref_mean
    signed = jnp.where(lax.bitwise_and(slot, 1) == 0, advantage, -advantage)
    pair = lax.shift_right_logical(slot, 1)
    margins = beta_scale * jnp.sum(jnp.where(pair == lane, signed, 0.0), axis=0, keepdims=True)
    softplus = jnp.maximum(-margins, 0.0) + jnp.log1p(jnp.exp(-jnp.abs(margins)))
    n_pairs = seqs // 2
    loss = jnp.sum(jnp.where(lane[:1] < n_pairs, softplus, 0.0), axis=1, keepdims=True) / n_pairs
    own_ref[...] = own
    margin_ref[...] = margins
    loss_ref[...] = jnp.broadcast_to(loss, margins.shape)


def fused(hidden, weight, targets, slot, prompt_len, ref_means):
    n_tok = lax.axis_size("tok")
    n_dev = n_tok * lax.axis_size("voc")
    rows = hidden.shape[0]
    cols, depth = weight.shape
    tile = plan_rows(cols)
    n_z = n_tok // 2
    whole = pl.BlockSpec(memory_space=pltpu.VMEM)
    wide = pl.BlockSpec(memory_space=pl.ANY)
    scalars = pl.BlockSpec(memory_space=pltpu.SMEM)
    ring = 4
    copies = 12 * n_z
    row = jax.ShapeDtypeStruct((1, rows), jnp.float32)
    own, margins, loss = pl.pallas_call(
        functools.partial(fused_kernel, n_tok, n_dev, tile),
        out_shape=(row, row, row),
        in_specs=[wide, wide, whole, scalars, scalars, scalars],
        out_specs=(whole, whole, whole),
        scratch_shapes=[
            pltpu.VMEM((rows * n_tok, depth), hidden.dtype),
            pltpu.VMEM((ring, 2 * tile, depth), weight.dtype),
            pltpu.VMEM((tile, 4 * rows), jnp.float32),
            pltpu.VMEM((tile, 4 * rows), jnp.float32),
            pltpu.VMEM((2 * tile, 2 * rows), jnp.float32),
            pltpu.VMEM((SUBS, 4 * rows), jnp.float32),
            pltpu.VMEM((SUBS, 4 * rows), jnp.float32),
            pltpu.VMEM((SUBS, 4 * rows), jnp.float32),
            pltpu.VMEM((n_dev // n_tok, n_z, 4, rows), jnp.float32),
            pltpu.VMEM((n_tok, n_z, 4, rows), jnp.float32),
            pltpu.VMEM((n_tok, rows), jnp.float32),
            pltpu.SemaphoreType.DMA((ring, 2)),
            pltpu.SemaphoreType.DMA,
            pltpu.SemaphoreType.DMA((copies,)),
            pltpu.SemaphoreType.DMA((copies,)),
            pltpu.SemaphoreType.DMA((n_dev // n_tok + n_tok,)),
            pltpu.SemaphoreType.DMA((n_dev // n_tok + n_tok,)),
        ],
        compiler_params=pltpu.CompilerParams(collective_id=3, has_side_effects=True, vmem_limit_bytes=63 * 1024 * 1024),
        cost_estimate=pl.CostEstimate(flops=2 * rows * n_tok * depth * cols, bytes_accessed=6 * depth * cols, transcendentals=rows * n_tok * cols),
    )(hidden, weight, targets.reshape(n_tok, rows), slot, prompt_len, ref_means)
    return own.reshape(-1), margins[0, : n_tok // 2], loss[0, 0]


def body(hidden, weight, targets, slot, prompt_len, ref_means):
    vocab_cols = weight.shape[1]
    n_tok = lax.axis_size("tok")
    rows, width = hidden.shape
    if lax.axis_size("voc") == 4 and n_tok == 8 and width % LANES == 0 and rows == LANES and vocab_cols >= 10 * plan_rows(vocab_cols) > 0:
        return fused(hidden, weight.T, targets, slot, prompt_len, ref_means)
    col_start = (lax.axis_index("voc") * lax.axis_size("tok") + lax.axis_index("tok")) * vocab_cols
    local = targets - col_start
    local = jnp.where((local >= 0) & (local < vocab_cols), local, -(1 << 30))
    wanted = jnp.broadcast_to(local[:, None], (targets.shape[0], LANES))
    stats = local_stats(gather_hidden(hidden), weight.T, wanted)
    return exchange_and_finish(stats, slot, prompt_len, ref_means)


def solution(mesh):
    in_specs = (P("tok", "voc"), P(None, ("voc", "tok")), P(), P(), P(), P())
    out_specs = (P("tok"), P(), P())
    return jax.shard_map(body, mesh=mesh, in_specs=in_specs, out_specs=out_specs, check_vma=False)
```
